8 devices in a mesh: graph: 8 (over z, y, x, core).
Axes of the slice: x: 2, y: 2, z: 1, core: 2. Of those that a mesh axis runs over, the one named last changes fastest.
Arguments:
- feats: bfloat16 [8192, 602], P('graph')
- w_one: float32 [602, 256], replicated
- w_two: float32 [256, 41], replicated
- send_idx: int32 [64, 64], P('graph')
- send_count: int32 [64], P('graph')
- edge_src: int32 [8192, 16], P('graph')
- edge_wt: float32 [8192, 16], P('graph')
- labels: int32 [8192], P('graph')
- label_mask: int32 [8192], P('graph')
Outputs:
- output 1: float32 [], replicated
- output 2: float32 [602, 256], replicated
- output 3: float32 [256, 41], replicated
All inputs are finite; a program needn't handle non-finite values.
Results may differ from the reference program's by a relative error of at most 0.00226.
Values are sent between devices in bfloat16 or wider.
A program may use at most 1 GiB of HBM per device.

```python
import jax
import jax.numpy as jnp
from jax import lax

GRAPH_DEVS = 8
ROWS_DEV = 1024
HALO_ROWS = 64
IN_DEG = 16
FEAT_IN = 602
FEAT_HID = 256
CLASSES = 41

TOTAL_ROWS = GRAPH_DEVS * ROWS_DEV
EXT_ROWS = ROWS_DEV + GRAPH_DEVS * HALO_ROWS


def draw_structure(rng_key):
    rng_keys = jax.random.split(rng_key, 7)
    dev_ids = jnp.arange(GRAPH_DEVS)
    skew_a = jax.random.randint(rng_keys[0], (GRAPH_DEVS, GRAPH_DEVS), 0, HALO_ROWS)
    skew_b = jax.random.randint(rng_keys[1], (GRAPH_DEVS, GRAPH_DEVS), 0, HALO_ROWS)
    counts = 1 + (skew_a * skew_b) // HALO_ROWS
    full_list = dev_ids[None, :] == (dev_ids[:, None] + 1) % GRAPH_DEVS
    counts = jnp.where(full_list, HALO_ROWS, counts)
    send_idx = jax.random.randint(rng_keys[2], (GRAPH_DEVS * GRAPH_DEVS, HALO_ROWS), 0, ROWS_DEV)
    edge_shape = (GRAPH_DEVS, ROWS_DEV, IN_DEG)
    is_cut = jax.random.randint(rng_keys[3], edge_shape, 0, 4) == 0
    local_src = jax.random.randint(rng_keys[4], edge_shape, 0, ROWS_DEV)
    peer_dev = (dev_ids[:, None, None] + jax.random.randint(rng_keys[5], edge_shape, 1, GRAPH_DEVS)) % GRAPH_DEVS
    peer_count = counts[peer_dev, dev_ids[:, None, None]]
    slot_pos = jax.random.randint(rng_keys[6], edge_shape, 0, 1048576) % peer_count
    halo_src = ROWS_DEV + peer_dev * HALO_ROWS + slot_pos
    edge_src = jnp.where(is_cut, halo_src, local_src).reshape(TOTAL_ROWS, IN_DEG)
    return send_idx, counts.reshape(GRAPH_DEVS * GRAPH_DEVS), edge_src, is_cut.reshape(TOTAL_ROWS, IN_DEG)


def setup_inputs(seed: int = 0) -> dict:
    rng_keys = jax.random.split(jax.random.key(seed), 7)
    feats = jax.random.normal(rng_keys[0], (TOTAL_ROWS, FEAT_IN), jnp.float32).astype(jnp.bfloat16)
    w_one = jax.random.normal(rng_keys[1], (FEAT_IN, FEAT_HID), jnp.float32) * FEAT_IN ** -0.5
    w_two = jax.random.normal(rng_keys[2], (FEAT_HID, CLASSES), jnp.float32) * FEAT_HID ** -0.5
    send_idx, send_count, edge_src, is_cut = draw_structure(rng_keys[3])
    raw_wt = jax.random.uniform(rng_keys[4], (TOTAL_ROWS, IN_DEG), jnp.float32, 0.5, 1.5) * jnp.where(is_cut, 0.5, 1.0)
    edge_wt = raw_wt / jnp.sqrt(jnp.sum(raw_wt * raw_wt, axis=1, keepdims=True))
    labels = jax.random.randint(rng_keys[5], (TOTAL_ROWS,), 0, CLASSES)
    label_mask = jax.random.randint(rng_keys[6], (TOTAL_ROWS,), 0, 2)
    return {"feats": feats, "w_one": w_one, "w_two": w_two, "send_idx": send_idx, "send_count": send_count, "edge_src": edge_src, "edge_wt": edge_wt, "labels": labels, "label_mask": label_mask}


def reference(feats, w_one, w_two, send_idx, send_count, edge_src, edge_wt, labels, label_mask):
    dev_ids = jnp.arange(GRAPH_DEVS)
    send_lists = send_idx.reshape(GRAPH_DEVS, GRAPH_DEVS, HALO_ROWS) + (dev_ids * ROWS_DEV)[:, None, None]
    is_valid = (jnp.arange(HALO_ROWS)[None, None, :] < send_count.reshape(GRAPH_DEVS, GRAPH_DEVS)[:, :, None]).astype(jnp.float32)
    halo_ids = jnp.transpose(send_lists, (1, 0, 2)).reshape(GRAPH_DEVS, GRAPH_DEVS * HALO_ROWS)
    halo_ok = jnp.transpose(is_valid, (1, 0, 2)).reshape(GRAPH_DEVS, GRAPH_DEVS * HALO_ROWS)
    src_dev = edge_src.reshape(GRAPH_DEVS, ROWS_DEV, IN_DEG)
    wt_dev = edge_wt.reshape(GRAPH_DEVS, ROWS_DEV, IN_DEG)

    def aggregate(h_flat):
        feat_width = h_flat.shape[1]

        def one_dev(per_dev):
            own_rows, src_ids, edge_w, ids_here, ok_here = per_dev
            halo_vals = h_flat[ids_here].astype(jnp.float32) * ok_here[:, None]
            ext_rows = jnp.concatenate([own_rows.astype(jnp.float32), halo_vals], axis=0)
            return jnp.sum(ext_rows[src_ids] * edge_w[:, :, None], axis=1)

        blocks = h_flat.reshape(GRAPH_DEVS, ROWS_DEV, feat_width)
        return lax.map(one_dev, (blocks, src_dev, wt_dev, halo_ids, halo_ok)).reshape(TOTAL_ROWS, feat_width)

    def scatter_back(d_z):
        feat_width = d_z.shape[1]

        def one_dev(per_dev):
            src_ids, edge_w, dz_rows = per_dev
            contrib = (edge_w[:, :, None] * dz_rows[:, None, :]).reshape(ROWS_DEV * IN_DEG, feat_width)
            return jax.ops.segment_sum(contrib, src_ids.reshape(ROWS_DEV * IN_DEG), num_segments=EXT_ROWS)

        ext_grad = lax.map(one_dev, (src_dev, wt_dev, d_z.reshape(GRAPH_DEVS, ROWS_DEV, feat_width)))
        own_grad = ext_grad[:, :ROWS_DEV].reshape(TOTAL_ROWS, feat_width)
        halo_grad = ext_grad[:, ROWS_DEV:] * halo_ok[:, :, None]
        back_sum = jax.ops.segment_sum(halo_grad.reshape(GRAPH_DEVS * GRAPH_DEVS * HALO_ROWS, feat_width), halo_ids.reshape(GRAPH_DEVS * GRAPH_DEVS * HALO_ROWS), num_segments=TOTAL_ROWS)
        return own_grad + back_sum

    w_one_b = w_one.astype(jnp.bfloat16)
    w_two_b = w_two.astype(jnp.bfloat16)
    z_one = aggregate(feats).astype(jnp.bfloat16)
    h_one = jnp.maximum(jnp.dot(z_one, w_one_b, preferred_element_type=jnp.float32), 0.0).astype(jnp.bfloat16)
    z_two = aggregate(h_one).astype(jnp.bfloat16)
    logits = jnp.dot(z_two, w_two_b, preferred_element_type=jnp.float32)
    mask_f = label_mask.astype(jnp.float32)
    label_total = jnp.sum(mask_f)
    log_prob = jax.nn.log_softmax(logits, axis=-1)
    onehot = (labels[:, None] == jnp.arange(CLASSES)[None, :]).astype(jnp.float32)
    loss_val = -jnp.sum(mask_f[:, None] * onehot * log_prob) / label_total
    d_logits = ((jnp.exp(log_prob) - onehot) * (mask_f / label_total)[:, None]).astype(jnp.bfloat16)
    grad_two = jnp.dot(z_two.T, d_logits, preferred_element_type=jnp.float32)
    d_z2 = jnp.dot(d_logits, w_two_b.T, preferred_element_type=jnp.float32)
    d_h1 = scatter_back(d_z2)
    d_y1 = jnp.where(h_one > 0, d_h1, 0.0).astype(jnp.bfloat16)
    grad_one = jnp.dot(z_one.T, d_y1, preferred_element_type=jnp.float32)
    return (loss_val, grad_one, grad_two)
```

```python
import jax
import jax.numpy as jnp
from jax import lax
from jax.experimental import pallas as pl
from jax.experimental.pallas import tpu as pltpu
from jax.sharding import PartitionSpec as P

MESH = pl.DeviceIdType.MESH
F32 = jnp.float32
BF16 = jnp.bfloat16

DEVS = 8
ROWS = 1024
HALO = 64
DEG = 16
EXT = ROWS + DEVS * HALO
FEAT = 602
FEAT_P = 608
FEAT_L = 640
HID = 256
CLS = 41
CLS_P = 48
OUT_SH = 168
LANE = 128
BUILD = 64


def dot_nn(a, b):
    return lax.dot_general(a, b, (((1,), (0,)), ((), ())), preferred_element_type=F32)


def dot_nt(a, b):
    return lax.dot_general(a, b, (((1,), (1,)), ((), ())), preferred_element_type=F32)


def split3(x):
    hi = x.astype(BF16)
    rest = x - hi.astype(F32)
    mid = rest.astype(BF16)
    low = (rest - mid.astype(F32)).astype(BF16)
    return hi, mid, low


def iota(shape, dim):
    return lax.broadcasted_iota(jnp.int32, shape, dim)


def kernel(feats_h, w_one_h, w_two_h, idx_ref, cnt_ref, src_ref, wt_ref, lab_ref, mask_ref,
           loss_ref, g1_ref, g2_ref,
           feats_raw, feats_t, w_one_f, w_two_f, w_two_p, w_one_t, wts, at_hi, at_mid, at_low, sel, sel_t,
           z1_acc, z1_t, h1_t, h1_n, x1, halo1, x2, halo2, th, tret, cnt_src, cnt_in,
           grads, a_in, b_out, b_in, outs,
           in_sem, s1, r1, sc, rc, s2, r2, s3, r3, sa, ra, sb, rb, so, ro, sd, rd):
    me = lax.axis_index("graph")
    core = me % 2
    chip = me // 2
    cx = chip % 2
    cy = chip // 2

    def flip_chip(f):
        fx, fy = f % 2, f // 2
        nx = 1 - cx if fx else cx
        ny = 1 - cy if fy else cy
        return ny * 2 + nx

    def flip_dev(f):
        nc = 1 - core if f % 2 else core
        return flip_chip(f // 2) * 2 + nc

    barrier = pltpu.get_barrier_semaphore()
    for f in range(1, DEVS):
        pl.semaphore_signal(barrier, inc=1, device_id=(flip_dev(f),), device_id_type=MESH)

    in_feats = pltpu.make_async_copy(feats_h, feats_raw, in_sem.at[0])
    in_one = pltpu.make_async_copy(w_one_h, w_one_f, in_sem.at[1])
    in_two = pltpu.make_async_copy(w_two_h, w_two_f, in_sem.at[2])
    in_feats.start()
    in_one.start()
    in_two.start()

    eye = iota((HALO, HALO), 0) == iota((HALO, HALO), 1)
    for q in range(DEVS):
        row = jnp.where(iota((1, HALO), 1) < cnt_ref[q], idx_ref[pl.ds(q, 1), :], -1).astype(F32)
        col = jnp.sum(jnp.where(eye, jnp.broadcast_to(row, (HALO, HALO)), 0.0), axis=1, keepdims=True)
        col = col.astype(jnp.int32)
        hot = iota((HALO, ROWS), 1) == jnp.broadcast_to(col, (HALO, ROWS))
        sel[pl.ds(q * HALO, HALO), :] = jnp.where(hot, 1.0, 0.0).astype(BF16)

    mask_f = mask_ref[...].astype(F32)
    own_count = jnp.sum(mask_f, axis=1, keepdims=True)
    cnt_src[...] = jnp.broadcast_to(own_count, (8, LANE))

    in_feats.wait()
    feats_t[pl.ds(592, FEAT_L - 592), :] = jnp.zeros((FEAT_L - 592, ROWS), BF16)
    feats_t[pl.ds(0, FEAT), :] = feats_raw[...]

    x1[...] = dot_nt(sel[...], feats_t[...]).astype(BF16)

    own_block = pl.ds(pl.multiple_of(me * HALO, HALO), HALO)
    halo1[own_block, :] = jnp.zeros((HALO, FEAT_L), BF16)
    halo2[own_block, :] = jnp.zeros((HALO, HID), BF16)
    tret[own_block, :] = jnp.zeros((HALO, LANE), F32)

    pl.semaphore_wait(barrier, DEVS - 1)

    def exchange(src, dst, send, recv):
        copies = []
        for f in range(1, DEVS):
            peer = flip_dev(f)
            copies.append(pltpu.make_async_remote_copy(
                src_ref=src.at[pl.ds(pl.multiple_of(peer * HALO, HALO), HALO), :],
                dst_ref=dst.at[own_block, :],
                send_sem=send.at[f], recv_sem=recv.at[f],
                device_id=(peer,), device_id_type=MESH))
        return copies

    order = [6, 7, 2, 3, 4, 5, 1]
    ex1 = exchange(x1, halo1, s1, r1)
    for f in order:
        ex1[f - 1].start()
    counts = []
    for f in range(1, DEVS):
        counts.append(pltpu.make_async_remote_copy(
            src_ref=cnt_src, dst_ref=cnt_in.at[f], send_sem=sc.at[f], recv_sem=rc.at[f],
            device_id=(flip_dev(f),), device_id_type=MESH))
        counts[-1].start()

    src = src_ref[...]
    wt = wt_ref[...]
    krow = iota((DEG, ROWS), 0)
    total = wt
    for d in range(1, DEG):
        same = (pltpu.roll(src, d, 0) == src) & (krow >= d)
        total = total + jnp.where(same, pltpu.roll(wt, d, 0), 0.0)
    wts[...] = total

    def build(s_first, s_count):
        def per_lane(t, carry):
            lanes = pl.ds(pl.multiple_of(t * LANE, LANE), LANE)
            src_b = src_ref[:, lanes]
            wt_b = wts[:, lanes]

            def per_rows(b, inner):
                start = pl.multiple_of(s_first + b * BUILD, BUILD)
                rel = src_b - start
                rows = iota((BUILD, LANE), 0)
                acc = jnp.zeros((BUILD, LANE), F32)
                for k in range(DEG):
                    hot = rows == jnp.broadcast_to(rel[k:k + 1, :], (BUILD, LANE))
                    acc = jnp.where(hot, jnp.broadcast_to(wt_b[k:k + 1, :], (BUILD, LANE)), acc)
                hi, mid, low = split3(acc)
                at_hi[pl.ds(start, BUILD), lanes] = hi
                at_mid[pl.ds(start, BUILD), lanes] = mid
                at_low[pl.ds(start, BUILD), lanes] = low
                return inner

            return lax.fori_loop(0, s_count // BUILD, per_rows, carry)

        lax.fori_loop(0, ROWS // LANE, per_lane, 0)

    build(0, ROWS)

    def aggregate(left, first, count, cols):
        rows = pl.ds(first, count)
        return (dot_nn(left, at_hi[rows, cols]) + dot_nn(left, at_mid[rows, cols])
                + dot_nn(left, at_low[rows, cols]))

    def cols_of(t):
        return pl.ds(t * 256, 256)

    for t in range(4):
        z1_acc[:, cols_of(t)] = aggregate(feats_t[pl.ds(0, FEAT_P), :], 0, ROWS, cols_of(t))

    build(ROWS, EXT - ROWS)
    sel_t[...] = sel[...].T

    in_one.wait()
    in_two.wait()
    w_one_t[:, pl.ds(512, FEAT_P - 512)] = jnp.zeros((HID, FEAT_P - 512), BF16)
    w_one_t[:, pl.ds(0, FEAT)] = w_one_f[...].T.astype(BF16)
    w_two_p[...] = jnp.zeros((CLS_P, HID), BF16)
    w_two_p[pl.ds(0, CLS), :] = w_two_f[...].astype(BF16)
    w_two_b = w_two_p[...]

    for f in order:
        ex1[f - 1].wait_recv()
    halo1_t = halo1[...].T[:FEAT_P, :]
    for t in range(4):
        z1_t[:, cols_of(t)] = (z1_acc[:, cols_of(t)]
                               + aggregate(halo1_t, ROWS, EXT - ROWS, cols_of(t))).astype(BF16)

    h1_t[...] = jnp.maximum(dot_nn(w_one_t[...], z1_t[...]), 0.0).astype(BF16)
    x2[...] = dot_nt(sel[...], h1_t[...]).astype(BF16)
    ex2 = exchange(x2, halo2, s2, r2)
    for f in order:
        ex2[f - 1].start()

    h1_n[...] = h1_t[...].T
    z2_acc = aggregate(h1_t[...], 0, ROWS, pl.ds(0, ROWS))
    for f in order:
        ex2[f - 1].wait_recv()
    z2_t = (z2_acc + aggregate(halo2[...].T, ROWS, EXT - ROWS, pl.ds(0, ROWS))).astype(BF16)

    count = cnt_src[...]
    for f in range(1, DEVS):
        counts[f - 1].wait_recv()
        count = count + cnt_in[f]
    count = count[0:1, 0:1]

    logits = dot_nn(w_two_b, z2_t)
    cls_row = iota((CLS_P, ROWS), 0)
    real = cls_row < CLS
    top = jnp.max(jnp.where(real, logits, -3.0e38), axis=0, keepdims=True)
    shifted = logits - top
    expo = jnp.where(real, jnp.exp(shifted), 0.0)
    log_prob = shifted - jnp.log(jnp.sum(expo, axis=0, keepdims=True))
    hit = cls_row == lab_ref[...]
    loss_row = jnp.sum(jnp.where(hit, log_prob, 0.0), axis=0, keepdims=True) * mask_f
    scale = mask_f / count
    d_log = (jnp.exp(log_prob) - jnp.where(hit, 1.0, 0.0)) * scale
    g2_t = jnp.where(real, d_log, 0.0).astype(BF16)
    g2_n = jnp.concatenate([g2_t.astype(F32), jnp.zeros((LANE - CLS_P, ROWS), F32)], axis=0).T.astype(BF16)

    def scatter(first, rows_n):
        rows = pl.ds(first, rows_n)
        return dot_nn(at_hi[rows, :], g2_n) + dot_nn(at_mid[rows, :], g2_n) + dot_nn(at_low[rows, :], g2_n)

    th[...] = scatter(ROWS, EXT - ROWS)
    ex3 = exchange(th, tret, s3, r3)
    for f in order:
        ex3[f - 1].start()

    own_t = scatter(0, ROWS)
    grad_two = dot_nt(g2_t, z2_t)
    loss_sum = jnp.sum(loss_row, axis=1, keepdims=True)
    grad_two = jnp.where(iota((CLS_P, HID), 0) == CLS, jnp.broadcast_to(loss_sum, (CLS_P, HID)), grad_two)
    w_stack = jnp.concatenate(
        [jnp.concatenate([w_two_b.astype(F32), jnp.zeros((LANE - CLS_P, HID), F32)], axis=0)] * 3, axis=0).astype(BF16)

    for f in order:
        ex3[f - 1].wait_recv()
    back = dot_nn(sel_t[...], jnp.concatenate(split3(tret[...]), axis=1))
    own_t = own_t + (back[:, 0:LANE] + back[:, LANE:2 * LANE] + back[:, 2 * LANE:3 * LANE])
    d_h1 = dot_nn(jnp.concatenate(split3(own_t), axis=1), w_stack)
    g1_b = jnp.where(h1_n[...].astype(F32) > 0, d_h1, 0.0).astype(BF16)
    grad_one = dot_nn(z1_t[...], g1_b)

    for h in range(2):
        lanes = slice(h * LANE, (h + 1) * LANE)
        for j in range(3):
            grads[h, j] = grad_one[j * OUT_SH:(j + 1) * OUT_SH, lanes]
        grads[h, 3, pl.ds(0, FEAT_P - 3 * OUT_SH), :] = grad_one[3 * OUT_SH:FEAT_P, lanes]
        grads[h, 3, pl.ds(FEAT_P - 3 * OUT_SH, CLS_P), :] = grad_two[:, lanes]
        grads[h, 3, pl.ds(FEAT_P - 3 * OUT_SH + CLS_P, 16), :] = jnp.zeros((16, LANE), F32)

    mate = flip_dev(1)
    flips = [3, 1, 2]
    copy_a = {}
    for o in flips + [0]:
        to_chip = flip_chip(o)
        copy_a[o] = pltpu.make_async_remote_copy(
            src_ref=grads.at[1 - core, to_chip], dst_ref=a_in.at[o], send_sem=sa.at[o], recv_sem=ra.at[o],
            device_id=(mate,), device_id_type=MESH)
        copy_a[o].start()
    copy_b = {}
    for o in flips:
        to_chip = flip_chip(o)
        copy_a[o].wait_recv()
        b_out[o] = grads[core, to_chip] + a_in[o]
        copy_b[o] = pltpu.make_async_remote_copy(
            src_ref=b_out.at[o], dst_ref=b_in.at[o], send_sem=sb.at[o], recv_sem=rb.at[o],
            device_id=(to_chip * 2 + core,), device_id_type=MESH)
        copy_b[o].start()
    copy_a[0].wait_recv()
    mine = grads[core, chip] + a_in[0]
    for o in flips:
        copy_b[o].wait_recv()
    mine = mine + ((b_in[1] + b_in[2]) + b_in[3])
    outs[core, chip] = mine
    copy_c = {}
    for o in flips:
        copy_c[o] = pltpu.make_async_remote_copy(
            src_ref=outs.at[core, chip], dst_ref=outs.at[core, chip], send_sem=so.at[o], recv_sem=ro.at[o],
            device_id=(flip_chip(o) * 2 + core,), device_id_type=MESH)
        copy_c[o].start()
    copy_d = {}
    for o in [0, 1, 2, 3]:
        at_chip = flip_chip(o)
        if o:
            copy_c[o].wait_recv()
        copy_d[o] = pltpu.make_async_remote_copy(
            src_ref=outs.at[core, at_chip], dst_ref=outs.at[core, at_chip], send_sem=sd.at[o], recv_sem=rd.at[o],
            device_id=(mate,), device_id_type=MESH)
        copy_d[o].start()
    for o in [0, 1, 2, 3]:
        copy_d[o].wait_recv()

    for h in range(2):
        lanes = pl.ds(h * LANE, LANE)
        for j in range(3):
            g1_ref[pl.ds(j * OUT_SH, OUT_SH), lanes] = outs[h, j]
        g1_ref[pl.ds(3 * OUT_SH, FEAT - 3 * OUT_SH), lanes] = outs[h, 3, 0:FEAT - 3 * OUT_SH, :]
        g2_ref[:, lanes] = outs[h, 3, FEAT_P - 3 * OUT_SH:FEAT_P - 3 * OUT_SH + CLS, :]
    loss_at = FEAT_P - 3 * OUT_SH + CLS
    loss_ref[...] = -outs[0, 3, loss_at:loss_at + 1, 0:1] / count

    for f in order:
        ex1[f - 1].wait_send()
        ex2[f - 1].wait_send()
        ex3[f - 1].wait_send()
        counts[f - 1].wait_send()
    for o in [0, 1, 2, 3]:
        copy_a[o].wait_send()
        copy_d[o].wait_send()
        if o:
            copy_b[o].wait_send()
            copy_c[o].wait_send()


def solution(mesh):
    vmem = pl.BlockSpec(memory_space=pltpu.VMEM)
    smem = pl.BlockSpec(memory_space=pltpu.SMEM)
    hbm = pl.BlockSpec(memory_space=pl.ANY)
    dma8 = pltpu.SemaphoreType.DMA((8,))
    dma4 = pltpu.SemaphoreType.DMA((4,))

    def device_step(feats, w_one, w_two, send_idx, send_count, edge_src, edge_wt, labels, label_mask):
        call = pl.pallas_call(
            kernel,
            out_shape=(jax.ShapeDtypeStruct((1, 1), F32), jax.ShapeDtypeStruct((FEAT, HID), F32),
                       jax.ShapeDtypeStruct((CLS, HID), F32)),
            in_specs=[hbm, hbm, hbm, vmem, smem, vmem, vmem, vmem, vmem],
            out_specs=(vmem, vmem, vmem),
            scratch_shapes=[
                pltpu.VMEM((FEAT, ROWS), BF16), pltpu.VMEM((FEAT_L, ROWS), BF16), pltpu.VMEM((FEAT, HID), F32),
                pltpu.VMEM((CLS, HID), F32), pltpu.VMEM((CLS_P, HID), BF16),
                pltpu.VMEM((HID, FEAT_P), BF16), pltpu.VMEM((DEG, ROWS), F32),
                pltpu.VMEM((EXT, ROWS), BF16), pltpu.VMEM((EXT, ROWS), BF16), pltpu.VMEM((EXT, ROWS), BF16),
                pltpu.VMEM((DEVS * HALO, ROWS), BF16), pltpu.VMEM((ROWS, DEVS * HALO), BF16),
                pltpu.VMEM((FEAT_P, ROWS), F32), pltpu.VMEM((FEAT_P, ROWS), BF16),
                pltpu.VMEM((HID, ROWS), BF16), pltpu.VMEM((ROWS, HID), BF16),
                pltpu.VMEM((DEVS * HALO, FEAT_L), BF16), pltpu.VMEM((DEVS * HALO, FEAT_L), BF16),
                pltpu.VMEM((DEVS * HALO, HID), BF16), pltpu.VMEM((DEVS * HALO, HID), BF16),
                pltpu.VMEM((DEVS * HALO, LANE), F32), pltpu.VMEM((DEVS * HALO, LANE), F32),
                pltpu.VMEM((8, LANE), F32), pltpu.VMEM((8, 8, LANE), F32),
                pltpu.VMEM((2, 4, OUT_SH, LANE), F32), pltpu.VMEM((4, OUT_SH, LANE), F32),
                pltpu.VMEM((4, OUT_SH, LANE), F32), pltpu.VMEM((4, OUT_SH, LANE), F32),
                pltpu.VMEM((2, 4, OUT_SH, LANE), F32),
                dma4, dma8, dma8, dma8, dma8, dma8, dma8, dma8, dma8,
                dma4, dma4, dma4, dma4, dma4, dma4, dma4, dma4,
            ],
            compiler_params=pltpu.CompilerParams(
                collective_id=0, has_side_effects=True, vmem_limit_bytes=56 * 1024 * 1024),
            name="gcn_step",
        )
        loss, grad_one, grad_two = call(
            feats.T, w_one, w_two.T, send_idx, send_count, edge_src.T, edge_wt.T,
            labels.reshape(1, ROWS), label_mask.reshape(1, ROWS))
        return loss.reshape(()), grad_one, grad_two.T

    row_spec = P("graph", None)
    vec_spec = P("graph")
    return jax.shard_map(
        device_step, mesh=mesh,
        in_specs=(row_spec, P(), P(), row_spec, vec_spec, row_spec, row_spec, vec_spec, vec_spec),
        out_specs=(P(), P(), P()), check_vma=False)
```

```python
import jax
import jax.numpy as jnp
from jax import lax
from jax.experimental import pallas as pl
from jax.experimental.pallas import tpu as pltpu
from jax.sharding import PartitionSpec as P

MESH = pl.DeviceIdType.MESH
F32 = jnp.float32
BF16 = jnp.bfloat16

DEVS = 8
ROWS = 1024
HALO = 64
DEG = 16
EXT = ROWS + (DEVS - 1) * HALO
FEAT = 602
FEAT_P = 608
FEAT_L = 640
HID = 256
CLS = 41
CLS_P = 48
OUT_SH = 168
LANE = 128
TILE = 512
TILES = ROWS // TILE
HALOS = (DEVS - 1) * HALO
SLOTS = [6, 7, 4, 1, 2, 5, 3]
EARLY = 4
SUBS = 3
SUB = OUT_SH // SUBS


def dot_nn(a, b):
    return lax.dot_general(a, b, (((1,), (0,)), ((), ())), preferred_element_type=F32)


def dot_nt(a, b):
    return lax.dot_general(a, b, (((1,), (1,)), ((), ())), preferred_element_type=F32)


def split3(x):
    hi = x.astype(BF16)
    rest = x - hi.astype(F32)
    mid = rest.astype(BF16)
    low = (rest - mid.astype(F32)).astype(BF16)
    return hi, mid, low


def iota(shape, dim):
    return lax.broadcasted_iota(jnp.int32, shape, dim)


def kernel(feats_h, w_one_h, w_two_h, idx_h, cnt_h, src_h, wt_h, lab_h, mask_h,
           loss_ref, g1_ref, g2_ref,
           idx_ref, cnt_ref, src_ref, wt_ref, lab_ref, mask_ref,
           feats_raw, feats_t, w_one_f, w_two_f, w_two_p, w_one_t, wts, row_ids, at_0, at_1, sel, sel_t,
           z1_acc, z1_t, z2_acc, z2_s, h1_t, h1_n, x1, halo1, x2, halo2, th, tret, cnt_src, cnt_in,
           grads, a_in, b_out, b_in, outs,
           in_sem, s1, r1, sc, rc, s2, r2, s3, r3, sa, ra, sb, rb, so, ro, sd, rd):
    me = lax.axis_index("graph")
    core = me % 2
    chip = me // 2
    cx = chip % 2
    cy = chip // 2

    def flip_chip(f):
        fx, fy = f % 2, f // 2
        nx = 1 - cx if fx else cx
        ny = 1 - cy if fy else cy
        return ny * 2 + nx

    def flip_dev(f):
        nc = 1 - core if f % 2 else core
        return flip_chip(f // 2) * 2 + nc

    peers = [flip_dev(f) for f in SLOTS]

    barrier = pltpu.get_barrier_semaphore()
    for peer in peers:
        pl.semaphore_signal(barrier, inc=1, device_id=(peer,), device_id_type=MESH)

    pairs = [(idx_h, idx_ref), (cnt_h, cnt_ref), (feats_h, feats_raw), (src_h, src_ref), (wt_h, wt_ref),
             (mask_h, mask_ref), (lab_h, lab_ref), (w_one_h, w_one_f), (w_two_h, w_two_f)]
    loads = [pltpu.make_async_copy(a, b, in_sem.at[n]) for n, (a, b) in enumerate(pairs)]
    for load in loads:
        load.start()
    ats = [at_0, at_1]

    row_ids[pl.ds(0, ROWS), :] = iota((ROWS, LANE), 0)
    for p, peer in enumerate(peers):
        row_ids[pl.ds(ROWS + p * HALO, HALO), :] = iota((HALO, LANE), 0) + (ROWS + peer * HALO)

    loads[0].wait()
    loads[1].wait()
    eye = iota((HALO, HALO), 0) == iota((HALO, HALO), 1)
    for p, peer in enumerate(peers):
        row = jnp.where(iota((1, HALO), 1) < cnt_ref[peer], idx_ref[pl.ds(peer, 1), :], -1).astype(F32)
        col = jnp.sum(jnp.where(eye, jnp.broadcast_to(row, (HALO, HALO)), 0.0), axis=1, keepdims=True)
        col = col.astype(jnp.int32)
        hot = iota((HALO, ROWS), 1) == jnp.broadcast_to(col, (HALO, ROWS))
        sel[pl.ds(p * HALO, HALO), :] = jnp.where(hot, 1.0, 0.0).astype(BF16)

    loads[5].wait()
    mask_f = mask_ref[...].astype(F32)
    own_count = jnp.sum(mask_f, axis=1, keepdims=True)
    cnt_src[...] = jnp.broadcast_to(own_count, (8, LANE))

    loads[3].wait()
    loads[4].wait()
    src = src_ref[...]
    wt = wt_ref[...]
    krow = iota((DEG, ROWS), 0)
    total = wt
    for d in range(1, DEG):
        same = (pltpu.roll(src, d, 0) == src) & (krow >= d)
        total = total + jnp.where(same, pltpu.roll(wt, d, 0), 0.0)
    wts[...] = total

    def build(t, half, start, count, step=32):
        for lane in range(2):
            at_lane = (half * 2 + lane) * LANE
            lanes = pl.ds(t * TILE + at_lane, LANE)
            source = src_ref[:, lanes]
            weight = wts[:, lanes]
            sources = [jnp.broadcast_to(source[k:k + 1, :], (step, LANE)) for k in range(DEG)]
            weights = [jnp.broadcast_to(weight[k:k + 1, :], (step, LANE)) for k in range(DEG)]
            for part in range(count // step):
                here = pl.ds(pl.multiple_of(start + part * step, step), step)
                rows = row_ids[here, :]
                acc = jnp.zeros((step, LANE), F32)
                for k in range(DEG):
                    acc = jnp.where(rows == sources[k], weights[k], acc)
                for n, term in enumerate(split3(acc)):
                    ats[t][n, here, pl.ds(at_lane, LANE)] = term

    def build_all(t, first, count, size):
        for half in range(2):
            def stage(i, carry, half=half):
                build(t, half, pl.multiple_of(first + i * size, size), size)
                return carry

            if count == size:
                build(t, half, first, size)
            else:
                lax.fori_loop(0, count // size, stage, 0)

    def aggregate(left, first, count, t):
        rows = pl.ds(first, count)
        return (dot_nn(left, ats[t][0, rows, :]) + dot_nn(left, ats[t][1, rows, :])
                + dot_nn(left, ats[t][2, rows, :]))

    def cols_of(t):
        return pl.ds(t * TILE, TILE)

    loads[2].wait()
    feats_t[pl.ds(592, FEAT_L - 592), :] = jnp.zeros((FEAT_L - 592, ROWS), BF16)
    feats_t[pl.ds(0, FEAT), :] = feats_raw[...]

    def exchange(src, dst, send, recv):
        return [pltpu.make_async_remote_copy(
            src_ref=src.at[pl.ds(p * HALO, HALO), :], dst_ref=dst.at[pl.ds(p * HALO, HALO), :],
            send_sem=send.at[p], recv_sem=recv.at[p], device_id=(peer,), device_id_type=MESH)
            for p, peer in enumerate(peers)]

    early = pl.ds(0, EARLY * HALO)
    late = pl.ds(EARLY * HALO, HALOS - EARLY * HALO)
    ex1 = exchange(x1, halo1, s1, r1)
    x1[early, :] = dot_nt(sel[early, :], feats_t[...]).astype(BF16)
    pl.semaphore_wait(barrier, DEVS - 1)
    for p in range(EARLY):
        ex1[p].start()
    x1[late, :] = dot_nt(sel[late, :], feats_t[...]).astype(BF16)
    for p in range(EARLY, DEVS - 1):
        ex1[p].start()
    counts = []
    for p, peer in enumerate(peers):
        counts.append(pltpu.make_async_remote_copy(
            src_ref=cnt_src, dst_ref=cnt_in.at[p], send_sem=sc.at[p], recv_sem=rc.at[p],
            device_id=(peer,), device_id_type=MESH))
        counts[-1].start()

    for t in range(TILES):
        build_all(t, 0, ROWS, 256)
        z1_acc[:, cols_of(t)] = aggregate(feats_t[pl.ds(0, FEAT_P), :], 0, ROWS, t)

    for t in range(TILES):
        build_all(t, ROWS, HALOS, 448)

    sel_t[...] = sel[...].T

    loads[6].wait()
    loads[7].wait()
    loads[8].wait()
    w_one_t[:, pl.ds(512, FEAT_P - 512)] = jnp.zeros((HID, FEAT_P - 512), BF16)
    w_one_t[:, pl.ds(0, FEAT)] = w_one_f[...].T.astype(BF16)
    w_two_p[...] = jnp.zeros((CLS_P, HID), BF16)
    w_two_p[pl.ds(0, CLS), :] = w_two_f[...].astype(BF16)
    w_two_b = w_two_p[...]
    w_stack = jnp.concatenate(
        [jnp.concatenate([w_two_b.astype(F32), jnp.zeros((LANE - CLS_P, HID), F32)], axis=0)] * 3, axis=0).astype(BF16)

    for p in range(EARLY):
        ex1[p].wait_recv()
    halo1_t = halo1[early, :].T[:FEAT_P, :]
    for t in range(TILES):
        z1_acc[:, cols_of(t)] = z1_acc[:, cols_of(t)] + aggregate(halo1_t, ROWS, EARLY * HALO, t)
    for p in range(EARLY, DEVS - 1):
        ex1[p].wait_recv()
    halo1_t = halo1[late, :].T[:FEAT_P, :]
    for t in range(TILES):
        z1_t[:, cols_of(t)] = (z1_acc[:, cols_of(t)] + aggregate(
            halo1_t, ROWS + EARLY * HALO, HALOS - EARLY * HALO, t)).astype(BF16)

    h1_t[...] = jnp.maximum(dot_nn(w_one_t[...], z1_t[...]), 0.0).astype(BF16)
    x2[...] = dot_nt(sel[...], h1_t[...]).astype(BF16)
    ex2 = exchange(x2, halo2, s2, r2)
    for copy in ex2:
        copy.start()

    h1_n[...] = h1_t[...].T
    for t in range(TILES):
        z2_acc[:, cols_of(t)] = aggregate(h1_t[...], 0, ROWS, t)
    for copy in ex2:
        copy.wait_recv()
    halo2_t = halo2[...].T
    for t in range(TILES):
        z2_s[:, cols_of(t)] = (z2_acc[:, cols_of(t)] + aggregate(halo2_t, ROWS, HALOS, t)).astype(BF16)
    z2_t = z2_s[...]

    count = cnt_src[...]
    for p in range(DEVS - 1):
        counts[p].wait_recv()
        count = count + cnt_in[p]
    count = count[0:1, 0:1]

    logits = dot_nn(w_two_b, z2_t)
    cls_row = iota((CLS_P, ROWS), 0)
    real = cls_row < CLS
    top = jnp.max(jnp.where(real, logits, -3.0e38), axis=0, keepdims=True)
    shifted = logits - top
    expo = jnp.where(real, jnp.exp(shifted), 0.0)
    log_prob = shifted - jnp.log(jnp.sum(expo, axis=0, keepdims=True))
    hit = cls_row == lab_ref[...]
    loss_row = jnp.sum(jnp.where(hit, log_prob, 0.0), axis=0, keepdims=True) * mask_f
    scale = mask_f / count
    d_log = (jnp.exp(log_prob) - jnp.where(hit, 1.0, 0.0)) * scale
    g2_t = jnp.where(real, d_log, 0.0).astype(BF16)
    g2_n = jnp.concatenate([g2_t.astype(F32), jnp.zeros((LANE - CLS_P, ROWS), F32)], axis=0).T.astype(BF16)

    def scatter(first, rows_n):
        rows = pl.ds(first, rows_n)
        out = jnp.zeros((rows_n, LANE), F32)
        for t in range(TILES):
            for n in range(3):
                out = out + dot_nn(ats[t][n, rows, :], g2_n[t * TILE:(t + 1) * TILE, :])
        return out

    th[...] = scatter(ROWS, HALOS)
    ex3 = exchange(th, tret, s3, r3)
    for copy in ex3:
        copy.start()

    own_t = scatter(0, ROWS)
    grad_two = dot_nt(g2_t, z2_t)
    loss_sum = jnp.sum(loss_row, axis=1, keepdims=True)
    grad_two = jnp.where(iota((CLS_P, HID), 0) == CLS, jnp.broadcast_to(loss_sum, (CLS_P, HID)), grad_two)

    for copy in ex3:
        copy.wait_recv()
    back = dot_nn(sel_t[...], jnp.concatenate(split3(tret[...]), axis=1))
    own_t = own_t + (back[:, 0:LANE] + back[:, LANE:2 * LANE] + back[:, 2 * LANE:3 * LANE])
    d_h1 = dot_nn(jnp.concatenate(split3(own_t), axis=1), w_stack)
    g1_b = jnp.where(h1_n[...].astype(F32) > 0, d_h1, 0.0).astype(BF16)
    grad_one = dot_nn(z1_t[...], g1_b)

    for h in range(2):
        lanes = slice(h * LANE, (h + 1) * LANE)
        for j in range(3):
            grads[h, j] = grad_one[j * OUT_SH:(j + 1) * OUT_SH, lanes]
        grads[h, 3, pl.ds(0, FEAT_P - 3 * OUT_SH), :] = grad_one[3 * OUT_SH:FEAT_P, lanes]
        grads[h, 3, pl.ds(FEAT_P - 3 * OUT_SH, CLS_P), :] = grad_two[:, lanes]
        grads[h, 3, pl.ds(FEAT_P - 3 * OUT_SH + CLS_P, 16), :] = jnp.zeros((16, LANE), F32)

    mate = flip_dev(1)
    flips = [3, 1, 2]

    def part(u):
        return pl.ds(u * SUB, SUB)

    copy_a, copy_b, copy_c, copy_d = {}, {}, {}, {}
    for u in range(SUBS):
        for o in flips + [0]:
            to_chip = flip_chip(o)
            copy_a[o, u] = pltpu.make_async_remote_copy(
                src_ref=grads.at[1 - core, to_chip, part(u), :], dst_ref=a_in.at[o, part(u), :],
                send_sem=sa.at[o, u], recv_sem=ra.at[o, u], device_id=(mate,), device_id_type=MESH)
            copy_a[o, u].start()
    for u in range(SUBS):
        for o in flips:
            to_chip = flip_chip(o)
            copy_a[o, u].wait_recv()
            b_out[o, part(u), :] = grads[core, to_chip, part(u), :] + a_in[o, part(u), :]
            copy_b[o, u] = pltpu.make_async_remote_copy(
                src_ref=b_out.at[o, part(u), :], dst_ref=b_in.at[o, part(u), :],
                send_sem=sb.at[o, u], recv_sem=rb.at[o, u],
                device_id=(to_chip * 2 + core,), device_id_type=MESH)
            copy_b[o, u].start()

    def to_mate(o, u):
        at_chip = flip_chip(o)
        copy_d[o, u] = pltpu.make_async_remote_copy(
            src_ref=outs.at[core, at_chip, part(u), :], dst_ref=outs.at[core, at_chip, part(u), :],
            send_sem=sd.at[o, u], recv_sem=rd.at[o, u], device_id=(mate,), device_id_type=MESH)
        copy_d[o, u].start()

    for u in range(SUBS):
        copy_a[0, u].wait_recv()
        mine = grads[core, chip, part(u), :] + a_in[0, part(u), :]
        for o in flips:
            copy_b[o, u].wait_recv()
        outs[core, chip, part(u), :] = mine + (
            (b_in[1, part(u), :] + b_in[2, part(u), :]) + b_in[3, part(u), :])
        for o in flips:
            copy_c[o, u] = pltpu.make_async_remote_copy(
                src_ref=outs.at[core, chip, part(u), :], dst_ref=outs.at[core, chip, part(u), :],
                send_sem=so.at[o, u], recv_sem=ro.at[o, u],
                device_id=(flip_chip(o) * 2 + core,), device_id_type=MESH)
            copy_c[o, u].start()
        to_mate(0, u)
    for u in range(SUBS):
        for o in [1, 2, 3]:
            copy_c[o, u].wait_recv()
            to_mate(o, u)
    for u in range(SUBS):
        for o in [0, 1, 2, 3]:
            copy_d[o, u].wait_recv()

    for h in range(2):
        lanes = pl.ds(h * LANE, LANE)
        for j in range(3):
            g1_ref[pl.ds(j * OUT_SH, OUT_SH), lanes] = outs[h, j]
        g1_ref[pl.ds(3 * OUT_SH, FEAT - 3 * OUT_SH), lanes] = outs[h, 3, 0:FEAT - 3 * OUT_SH, :]
        g2_ref[:, lanes] = outs[h, 3, FEAT_P - 3 * OUT_SH:FEAT_P - 3 * OUT_SH + CLS, :]
    loss_at = FEAT_P - 3 * OUT_SH + CLS
    loss_ref[...] = -outs[0, 3, loss_at:loss_at + 1, 0:1] / count

    for copy in ex1 + ex2 + ex3 + counts:
        copy.wait_send()
    for group in (copy_a, copy_b, copy_c, copy_d):
        for copy in group.values():
            copy.wait_send()


def solution(mesh):
    vmem = pl.BlockSpec(memory_space=pltpu.VMEM)
    hbm = pl.BlockSpec(memory_space=pl.ANY)
    dma8 = pltpu.SemaphoreType.DMA((8,))
    dma_sum = pltpu.SemaphoreType.DMA((4, SUBS))

    def device_step(feats, w_one, w_two, send_idx, send_count, edge_src, edge_wt, labels, label_mask):
        call = pl.pallas_call(
            kernel,
            out_shape=(pltpu.VMEM((1, 1), F32), pltpu.VMEM((FEAT, HID), F32),
                       pltpu.VMEM((CLS, HID), F32)),
            in_specs=[hbm] * 9,
            out_specs=(vmem, vmem, vmem),
            scratch_shapes=[
                pltpu.VMEM((DEVS, HALO), jnp.int32), pltpu.SMEM((DEVS,), jnp.int32),
                pltpu.VMEM((DEG, ROWS), jnp.int32), pltpu.VMEM((DEG, ROWS), F32),
                pltpu.VMEM((1, ROWS), jnp.int32), pltpu.VMEM((1, ROWS), jnp.int32),
                pltpu.VMEM((FEAT, ROWS), BF16), pltpu.VMEM((FEAT_L, ROWS), BF16), pltpu.VMEM((FEAT, HID), F32),
                pltpu.VMEM((CLS, HID), F32), pltpu.VMEM((CLS_P, HID), BF16),
                pltpu.VMEM((HID, FEAT_P), BF16), pltpu.VMEM((DEG, ROWS), F32), pltpu.VMEM((EXT, LANE), jnp.int32),
                pltpu.VMEM((3, EXT, TILE), BF16), pltpu.VMEM((3, EXT, TILE), BF16),
                pltpu.VMEM((HALOS, ROWS), BF16), pltpu.VMEM((ROWS, HALOS), BF16),
                pltpu.VMEM((FEAT_P, ROWS), F32), pltpu.VMEM((FEAT_P, ROWS), BF16),
                pltpu.VMEM((HID, ROWS), F32), pltpu.VMEM((HID, ROWS), BF16),
                pltpu.VMEM((HID, ROWS), BF16), pltpu.VMEM((ROWS, HID), BF16),
                pltpu.VMEM((HALOS, FEAT_L), BF16), pltpu.VMEM((HALOS, FEAT_L), BF16),
                pltpu.VMEM((HALOS, HID), BF16), pltpu.VMEM((HALOS, HID), BF16),
                pltpu.VMEM((HALOS, LANE), F32), pltpu.VMEM((HALOS, LANE), F32),
                pltpu.VMEM((8, LANE), F32), pltpu.VMEM((8, 8, LANE), F32),
                pltpu.VMEM((2, 4, OUT_SH, LANE), F32), pltpu.VMEM((4, OUT_SH, LANE), F32),
                pltpu.VMEM((4, OUT_SH, LANE), F32), pltpu.VMEM((4, OUT_SH, LANE), F32),
                pltpu.VMEM((2, 4, OUT_SH, LANE), F32),
                pltpu.SemaphoreType.DMA((9,)), dma8, dma8, dma8, dma8, dma8, dma8, dma8, dma8,
                dma_sum, dma_sum, dma_sum, dma_sum, dma_sum, dma_sum, dma_sum, dma_sum,
            ],
            compiler_params=pltpu.CompilerParams(
                collective_id=0, has_side_effects=True, vmem_limit_bytes=56 * 1024 * 1024),
            name="gcn_step",
        )
        loss, grad_one, grad_two = call(
            feats.T, w_one, w_two.T, send_idx, send_count, edge_src.T, edge_wt.T,
            labels.reshape(1, ROWS), label_mask.reshape(1, ROWS))
        return loss.reshape(()), grad_one, grad_two.T

    row_spec = P("graph", None)
    vec_spec = P("graph")
    return jax.shard_map(
        device_step, mesh=mesh,
        in_specs=(row_spec, P(), P(), row_spec, vec_spec, row_spec, row_spec, vec_spec, vec_spec),
        out_specs=(P(), P(), P()), check_vma=False)
```

```python
import jax
import jax.numpy as jnp
from jax import lax
from jax.experimental import pallas as pl
from jax.experimental.pallas import tpu as pltpu
from jax.sharding import PartitionSpec as P

MESH = pl.DeviceIdType.MESH
F32 = jnp.float32
BF16 = jnp.bfloat16

DEVS = 8
ROWS = 1024
HALO = 64
DEG = 16
EXT = ROWS + (DEVS - 1) * HALO
FEAT = 602
FEAT_P = 608
FEAT_L = 640
HID = 256
CLS = 41
CLS_P = 48
OUT_SH = 168
LANE = 128
TILE = 512
TILES = ROWS // TILE
HALOS = (DEVS - 1) * HALO
SLOTS = [6, 7, 4, 5, 2, 3, 1]
EARLY = 4
SUBS = 3
SUB = OUT_SH // SUBS


def dot_nn(a, b):
    return lax.dot_general(a, b, (((1,), (0,)), ((), ())), preferred_element_type=F32)


def dot_nt(a, b):
    return lax.dot_general(a, b, (((1,), (1,)), ((), ())), preferred_element_type=F32)


def split3(x):
    hi = x.astype(BF16)
    rest = x - hi.astype(F32)
    mid = rest.astype(BF16)
    low = (rest - mid.astype(F32)).astype(BF16)
    return hi, mid, low


def iota(shape, dim):
    return lax.broadcasted_iota(jnp.int32, shape, dim)


def kernel(feats_h, w_one_h, w_two_h, idx_h, cnt_h, src_h, wt_h, lab_h, mask_h,
           loss_ref, g1_ref, g2_ref,
           idx_ref, cnt_ref, src_ref, wt_ref, lab_ref, mask_ref,
           feats_raw, feats_t, w_one_f, w_two_f, w_two_p, w_two_3, w_one_t, wts, row_ids, at_0, at_1, sel,
           z1_acc, z1_t, z2_acc, z2_s, h1_t, x1, halo1, x2, halo2, th, tret, cnt_src, cnt_in,
           grads, a_in, b_out, b_in, outs,
           in_sem, s1, r1, sc, rc, s2, r2, s3, r3, sa, ra, sb, rb, so, ro, sd, rd):
    me = lax.axis_index("graph")
    core = me % 2
    chip = me // 2
    cx = chip % 2
    cy = chip // 2

    def flip_chip(f):
        fx, fy = f % 2, f // 2
        nx = 1 - cx if fx else cx
        ny = 1 - cy if fy else cy
        return ny * 2 + nx

    def flip_dev(f):
        nc = 1 - core if f % 2 else core
        return flip_chip(f // 2) * 2 + nc

    peers = [flip_dev(f) for f in SLOTS]

    barrier = pltpu.get_barrier_semaphore()
    for peer in peers:
        pl.semaphore_signal(barrier, inc=1, device_id=(peer,), device_id_type=MESH)

    pairs = [(idx_h, idx_ref), (cnt_h, cnt_ref), (feats_h, feats_raw), (src_h, src_ref), (wt_h, wt_ref),
             (mask_h, mask_ref), (lab_h, lab_ref), (w_one_h, w_one_f), (w_two_h, w_two_f)]
    loads = [pltpu.make_async_copy(a, b, in_sem.at[n]) for n, (a, b) in enumerate(pairs)]
    for load in loads:
        load.start()
    ats = [at_0, at_1]

    def number_rows(i, carry):
        start = pl.multiple_of(i * 32, 32)
        row_ids[pl.ds(start, 32), :] = iota((32, LANE), 0) + start
        return carry

    lax.fori_loop(0, ROWS // 32, number_rows, 0)
    for p, peer in enumerate(peers):
        def number_halo(i, carry, p=p, peer=peer):
            start = pl.multiple_of(i * 32, 32)
            row_ids[pl.ds(ROWS + p * HALO + start, 32), :] = iota((32, LANE), 0) + (ROWS + peer * HALO + start)
            return carry

        lax.fori_loop(0, HALO // 32, number_halo, 0)

    loads[0].wait()
    loads[1].wait()
    eye = iota((HALO, HALO), 0) == iota((HALO, HALO), 1)
    for p, peer in enumerate(peers):
        row = jnp.where(iota((1, HALO), 1) < cnt_ref[peer], idx_ref[pl.ds(peer, 1), :], -1).astype(F32)
        col = jnp.sum(jnp.where(eye, jnp.broadcast_to(row, (HALO, HALO)), 0.0), axis=1, keepdims=True)
        col = col.astype(jnp.int32)
        hot = iota((HALO, ROWS), 1) == jnp.broadcast_to(col, (HALO, ROWS))
        sel[pl.ds(p * HALO, HALO), :] = jnp.where(hot, 1.0, 0.0).astype(BF16)

    loads[5].wait()
    mask_f = mask_ref[...].astype(F32)
    own_count = jnp.sum(mask_f, axis=1, keepdims=True)
    cnt_src[...] = jnp.broadcast_to(own_count, (8, LANE))

    loads[3].wait()
    loads[4].wait()
    src = src_ref[...]
    wt = wt_ref[...]
    krow = iota((DEG, ROWS), 0)
    total = wt
    for d in range(1, DEG):
        same = (pltpu.roll(src, d, 0) == src) & (krow >= d)
        total = total + jnp.where(same, pltpu.roll(wt, d, 0), 0.0)
    wts[...] = total

    def build(t, lane, start, count, step=32):
        lanes = pl.ds(pl.multiple_of(t * TILE + lane * LANE, LANE), LANE)
        source = src_ref[:, lanes]
        weight = wts[:, lanes]
        sources = [jnp.broadcast_to(source[k:k + 1, :], (step, LANE)) for k in range(DEG)]
        weights = [jnp.broadcast_to(weight[k:k + 1, :], (step, LANE)) for k in range(DEG)]
        for piece in range(count // step):
            here = pl.ds(pl.multiple_of(start + piece * step, step), step)
            rows = row_ids[here, :]
            acc = jnp.zeros((step, LANE), F32)
            for k in range(DEG):
                acc = jnp.where(rows == sources[k], weights[k], acc)
            for n, term in enumerate(split3(acc)):
                ats[t][n, here, pl.ds(pl.multiple_of(lane * LANE, LANE), LANE)] = term

    def build_local(t):
        def stage(i, carry):
            build(t, i // 2, pl.multiple_of((i % 2) * 512, 512), 512)
            return carry

        lax.fori_loop(0, 8, stage, 0)

    def build_halo(t):
        def stage(i, carry):
            build(t, i, ROWS, HALOS)
            return carry

        lax.fori_loop(0, 4, stage, 0)

    def aggregate(left, first, count, t):
        rows = pl.ds(first, count)
        return (dot_nn(left, ats[t][0, rows, :]) + dot_nn(left, ats[t][1, rows, :])
                + dot_nn(left, ats[t][2, rows, :]))

    def cols_of(t):
        return pl.ds(t * TILE, TILE)

    loads[2].wait()
    feats_t[pl.ds(592, FEAT_L - 592), :] = jnp.zeros((FEAT_L - 592, ROWS), BF16)
    feats_t[pl.ds(0, FEAT), :] = feats_raw[...]

    def exchange(src, dst, send, recv):
        return [pltpu.make_async_remote_copy(
            src_ref=src.at[pl.ds(p * HALO, HALO), :], dst_ref=dst.at[pl.ds(p * HALO, HALO), :],
            send_sem=send.at[p], recv_sem=recv.at[p], device_id=(peer,), device_id_type=MESH)
            for p, peer in enumerate(peers)]

    early = pl.ds(0, EARLY * HALO)
    late = pl.ds(EARLY * HALO, HALOS - EARLY * HALO)
    ex1 = exchange(x1, halo1, s1, r1)
    x1[early, :] = dot_nt(sel[early, :], feats_t[...]).astype(BF16)
    pl.semaphore_wait(barrier, DEVS - 1)
    for p in range(EARLY):
        ex1[p].start()
    x1[late, :] = dot_nt(sel[late, :], feats_t[...]).astype(BF16)
    for p in range(EARLY, DEVS - 1):
        ex1[p].start()
    counts = []
    for p, peer in enumerate(peers):
        counts.append(pltpu.make_async_remote_copy(
            src_ref=cnt_src, dst_ref=cnt_in.at[p], send_sem=sc.at[p], recv_sem=rc.at[p],
            device_id=(peer,), device_id_type=MESH))
        counts[-1].start()

    for t in range(TILES):
        build_local(t)
        z1_acc[:, cols_of(t)] = aggregate(feats_t[pl.ds(0, FEAT_P), :], 0, ROWS, t)

    for t in range(TILES):
        build_halo(t)

    loads[6].wait()
    loads[7].wait()
    loads[8].wait()
    w_one_t[:, pl.ds(512, FEAT_P - 512)] = jnp.zeros((HID, FEAT_P - 512), BF16)
    w_one_t[:, pl.ds(0, FEAT)] = w_one_f[...].T.astype(BF16)
    w_two_p[...] = jnp.zeros((CLS_P, HID), BF16)
    w_two_p[pl.ds(0, CLS), :] = w_two_f[...].astype(BF16)
    w_two_b = w_two_p[...]

    for p in range(EARLY):
        ex1[p].wait_recv()
    halo1_t = halo1[early, :].T[:FEAT_P, :]
    for t in range(TILES):
        z1_acc[:, cols_of(t)] = z1_acc[:, cols_of(t)] + aggregate(halo1_t, ROWS, EARLY * HALO, t)
    for p in range(EARLY, DEVS - 1):
        ex1[p].wait_recv()
    halo1_t = halo1[late, :].T[:FEAT_P, :]
    for t in range(TILES):
        z1_t[:, cols_of(t)] = (z1_acc[:, cols_of(t)] + aggregate(
            halo1_t, ROWS + EARLY * HALO, HALOS - EARLY * HALO, t)).astype(BF16)

    h1_t[...] = jnp.maximum(dot_nn(w_one_t[...], z1_t[...]), 0.0).astype(BF16)
    for part_rows in (pl.ds(0, HALOS // 2), pl.ds(HALOS // 2, HALOS // 2)):
        x2[part_rows, :] = dot_nt(sel[part_rows, :], h1_t[...]).astype(BF16)
    ex2 = exchange(x2, halo2, s2, r2)
    for copy in ex2:
        copy.start()

    w_two_3[...] = jnp.concatenate([w_two_b.astype(F32)] * 3, axis=0).T.astype(BF16)
    for t in range(TILES):
        z2_acc[:, cols_of(t)] = aggregate(h1_t[...], 0, ROWS, t)
    for copy in ex2:
        copy.wait_recv()
    halo2_t = halo2[...].T
    for t in range(TILES):
        z2_s[:, cols_of(t)] = (z2_acc[:, cols_of(t)] + aggregate(halo2_t, ROWS, HALOS, t)).astype(BF16)
    z2_t = z2_s[...]

    count = cnt_src[...]
    for p in range(DEVS - 1):
        counts[p].wait_recv()
        count = count + cnt_in[p]
    count = count[0:1, 0:1]

    logits = dot_nn(w_two_b, z2_t)
    cls_row = iota((CLS_P, ROWS), 0)
    real = cls_row < CLS
    top = jnp.max(jnp.where(real, logits, -3.0e38), axis=0, keepdims=True)
    shifted = logits - top
    expo = jnp.where(real, jnp.exp(shifted), 0.0)
    log_prob = shifted - jnp.log(jnp.sum(expo, axis=0, keepdims=True))
    hit = cls_row == lab_ref[...]
    loss_row = jnp.sum(jnp.where(hit, log_prob, 0.0), axis=0, keepdims=True) * mask_f
    scale = mask_f / count
    d_log = (jnp.exp(log_prob) - jnp.where(hit, 1.0, 0.0)) * scale
    g2_t = jnp.where(real, d_log, 0.0).astype(BF16)

    def scatter(first, rows_n):
        rows = pl.ds(first, rows_n)
        out = jnp.zeros((CLS_P, rows_n), F32)
        for t in range(TILES):
            for n in range(3):
                out = out + dot_nt(g2_t[:, t * TILE:(t + 1) * TILE], ats[t][n, rows, :])
        return out

    th[:, pl.ds(0, HALOS)] = scatter(ROWS, HALOS)
    th[:, pl.ds(HALOS, HALO)] = jnp.zeros((CLS_P, HALO), F32)
    ex3 = [pltpu.make_async_remote_copy(
        src_ref=th.at[:, pl.ds(p // 2 * LANE, LANE)], dst_ref=tret.at[p],
        send_sem=s3.at[p], recv_sem=r3.at[p], device_id=(peer,), device_id_type=MESH)
        for p, peer in enumerate(peers)]
    for copy in ex3:
        copy.start()

    own_t = scatter(0, ROWS)
    grad_two = dot_nt(g2_t, z2_t)
    loss_sum = jnp.sum(loss_row, axis=1, keepdims=True)
    grad_two = jnp.where(iota((CLS_P, HID), 0) == CLS, jnp.broadcast_to(loss_sum, (CLS_P, HID)), grad_two)

    for copy in ex3:
        copy.wait_recv()
    first_half = iota((CLS_P, LANE), 1) < HALO
    blocks = [jnp.where(first_half, tret[2 * n], tret[2 * n + 1] if n < 3 else 0.0) for n in range(4)]
    back_t = jnp.concatenate(blocks, axis=1)[:, :HALOS]
    back = dot_nn(jnp.concatenate(split3(back_t), axis=0), sel[...])
    own_t = own_t + (back[0:CLS_P] + back[CLS_P:2 * CLS_P] + back[2 * CLS_P:3 * CLS_P])
    d_h1 = dot_nn(w_two_3[...], jnp.concatenate(split3(own_t), axis=0))
    g1_b = jnp.where(h1_t[...].astype(F32) > 0, d_h1, 0.0).astype(BF16)
    half_m = FEAT_P // 2
    grad_one = jnp.concatenate([dot_nt(z1_t[pl.ds(0, half_m), :], g1_b),
                                dot_nt(z1_t[pl.ds(half_m, half_m), :], g1_b)], axis=0)

    for h in range(2):
        lanes = slice(h * LANE, (h + 1) * LANE)
        for j in range(3):
            grads[h, j] = grad_one[j * OUT_SH:(j + 1) * OUT_SH, lanes]
        grads[h, 3, pl.ds(0, FEAT_P - 3 * OUT_SH), :] = grad_one[3 * OUT_SH:FEAT_P, lanes]
        grads[h, 3, pl.ds(FEAT_P - 3 * OUT_SH, CLS_P), :] = grad_two[:, lanes]
        grads[h, 3, pl.ds(FEAT_P - 3 * OUT_SH + CLS_P, 16), :] = jnp.zeros((16, LANE), F32)

    mate = flip_dev(1)
    flips = [3, 1, 2]

    def part(u):
        return pl.ds(u * SUB, SUB)

    copy_a, copy_b, copy_c, copy_d = {}, {}, {}, {}
    for u in range(SUBS):
        for o in flips + [0]:
            to_chip = flip_chip(o)
            copy_a[o, u] = pltpu.make_async_remote_copy(
                src_ref=grads.at[1 - core, to_chip, part(u), :], dst_ref=a_in.at[o, part(u), :],
                send_sem=sa.at[o, u], recv_sem=ra.at[o, u], device_id=(mate,), device_id_type=MESH)
            copy_a[o, u].start()
    for u in range(SUBS):
        for o in flips:
            to_chip = flip_chip(o)
            copy_a[o, u].wait_recv()
            b_out[o, part(u), :] = grads[core, to_chip, part(u), :] + a_in[o, part(u), :]
            copy_b[o, u] = pltpu.make_async_remote_copy(
                src_ref=b_out.at[o, part(u), :], dst_ref=b_in.at[o, part(u), :],
                send_sem=sb.at[o, u], recv_sem=rb.at[o, u],
                device_id=(to_chip * 2 + core,), device_id_type=MESH)
            copy_b[o, u].start()

    def to_mate(o, u):
        at_chip = flip_chip(o)
        copy_d[o, u] = pltpu.make_async_remote_copy(
            src_ref=outs.at[core, at_chip, part(u), :], dst_ref=outs.at[core, at_chip, part(u), :],
            send_sem=sd.at[o, u], recv_sem=rd.at[o, u], device_id=(mate,), device_id_type=MESH)
        copy_d[o, u].start()

    for u in range(SUBS):
        copy_a[0, u].wait_recv()
        mine = grads[core, chip, part(u), :] + a_in[0, part(u), :]
        for o in flips:
            copy_b[o, u].wait_recv()
        outs[core, chip, part(u), :] = mine + (
            (b_in[1, part(u), :] + b_in[2, part(u), :]) + b_in[3, part(u), :])
        for o in flips:
            copy_c[o, u] = pltpu.make_async_remote_copy(
                src_ref=outs.at[core, chip, part(u), :], dst_ref=outs.at[core, chip, part(u), :],
                send_sem=so.at[o, u], recv_sem=ro.at[o, u],
                device_id=(flip_chip(o) * 2 + core,), device_id_type=MESH)
            copy_c[o, u].start()
        to_mate(0, u)
    for u in range(SUBS):
        for o in [1, 2, 3]:
            copy_c[o, u].wait_recv()
            to_mate(o, u)
    for u in range(SUBS):
        for o in [0, 1, 2, 3]:
            copy_d[o, u].wait_recv()

    for h in range(2):
        lanes = pl.ds(h * LANE, LANE)
        for j in range(3):
            g1_ref[pl.ds(j * OUT_SH, OUT_SH), lanes] = outs[h, j]
        g1_ref[pl.ds(3 * OUT_SH, FEAT - 3 * OUT_SH), lanes] = outs[h, 3, 0:FEAT - 3 * OUT_SH, :]
        g2_ref[:, lanes] = outs[h, 3, FEAT_P - 3 * OUT_SH:FEAT_P - 3 * OUT_SH + CLS, :]
    loss_at = FEAT_P - 3 * OUT_SH + CLS
    loss_ref[...] = -outs[0, 3, loss_at:loss_at + 1, 0:1] / count

    for copy in ex1 + ex2 + ex3 + counts:
        copy.wait_send()
    for group in (copy_a, copy_b, copy_c, copy_d):
        for copy in group.values():
            copy.wait_send()


def solution(mesh):
    vmem = pl.BlockSpec(memory_space=pltpu.VMEM)
    hbm = pl.BlockSpec(memory_space=pl.ANY)
    dma8 = pltpu.SemaphoreType.DMA((8,))
    dma_sum = pltpu.SemaphoreType.DMA((4, SUBS))

    def device_step(feats, w_one, w_two, send_idx, send_count, edge_src, edge_wt, labels, label_mask):
        call = pl.pallas_call(
            kernel,
            out_shape=(pltpu.VMEM((1, 1), F32), pltpu.VMEM((FEAT, HID), F32),
                       pltpu.VMEM((CLS, HID), F32)),
            in_specs=[hbm] * 9,
            out_specs=(vmem, vmem, vmem),
            scratch_shapes=[
                pltpu.VMEM((DEVS, HALO), jnp.int32), pltpu.SMEM((DEVS,), jnp.int32),
                pltpu.VMEM((DEG, ROWS), jnp.int32), pltpu.VMEM((DEG, ROWS), F32),
                pltpu.VMEM((1, ROWS), jnp.int32), pltpu.VMEM((1, ROWS), jnp.int32),
                pltpu.VMEM((FEAT, ROWS), BF16), pltpu.VMEM((FEAT_L, ROWS), BF16), pltpu.VMEM((FEAT, HID), F32),
                pltpu.VMEM((CLS, HID), F32), pltpu.VMEM((CLS_P, HID), BF16), pltpu.VMEM((HID, 3 * CLS_P), BF16),
                pltpu.VMEM((HID, FEAT_P), BF16), pltpu.VMEM((DEG, ROWS), F32), pltpu.VMEM((EXT, LANE), jnp.int32),
                pltpu.VMEM((3, EXT, TILE), BF16), pltpu.VMEM((3, EXT, TILE), BF16),
                pltpu.VMEM((HALOS, ROWS), BF16),
                pltpu.VMEM((FEAT_P, ROWS), F32), pltpu.VMEM((FEAT_P, ROWS), BF16),
                pltpu.VMEM((HID, ROWS), F32), pltpu.VMEM((HID, ROWS), BF16),
                pltpu.VMEM((HID, ROWS), BF16),
                pltpu.VMEM((HALOS, FEAT_L), BF16), pltpu.VMEM((HALOS, FEAT_L), BF16),
                pltpu.VMEM((HALOS, HID), BF16), pltpu.VMEM((HALOS, HID), BF16),
                pltpu.VMEM((CLS_P, 512), F32), pltpu.VMEM((7, CLS_P, LANE), F32),
                pltpu.VMEM((8, LANE), F32), pltpu.VMEM((8, 8, LANE), F32),
                pltpu.VMEM((2, 4, OUT_SH, LANE), F32), pltpu.VMEM((4, OUT_SH, LANE), F32),
                pltpu.VMEM((4, OUT_SH, LANE), F32), pltpu.VMEM((4, OUT_SH, LANE), F32),
                pltpu.VMEM((2, 4, OUT_SH, LANE), F32),
                pltpu.SemaphoreType.DMA((9,)), dma8, dma8, dma8, dma8, dma8, dma8, dma8, dma8,
                dma_sum, dma_sum, dma_sum, dma_sum, dma_sum, dma_sum, dma_sum, dma_sum,
            ],
            compiler_params=pltpu.CompilerParams(
                collective_id=0, has_side_effects=True, vmem_limit_bytes=56 * 1024 * 1024),
            name="gcn_step",
        )
        loss, grad_one, grad_two = call(
            feats.T, w_one, w_two.T, send_idx, send_count, edge_src.T, edge_wt.T,
            labels.reshape(1, ROWS), label_mask.reshape(1, ROWS))
        return loss.reshape(()), grad_one, grad_two.T

    row_spec = P("graph", None)
    vec_spec = P("graph")
    return jax.shard_map(
        device_step, mesh=mesh,
        in_specs=(row_spec, P(), P(), row_spec, vec_spec, row_spec, row_spec, vec_spec, vec_spec),
        out_specs=(P(), P(), P()), check_vma=False)
```

```python
import jax
import jax.numpy as jnp
from jax import lax
from jax.experimental import pallas as pl
from jax.experimental.pallas import tpu as pltpu
from jax.sharding import PartitionSpec as P

MESH = pl.DeviceIdType.MESH
F32 = jnp.float32
BF16 = jnp.bfloat16

DEVS = 8
ROWS = 1024
HALO = 64
DEG = 16
EXT = ROWS + (DEVS - 1) * HALO
FEAT = 602
FEAT_P = 608
FEAT_L = 640
HID = 256
CLS = 41
CLS_P = 48
OUT_SH = 168
LANE = 128
TILE = 512
TILES = ROWS // TILE
HALOS = (DEVS - 1) * HALO
SLOTS = [6, 7, 4, 5, 2, 3, 1]
EARLY = 4
SUBS = 3
AHEAD = 2
SUB = OUT_SH // SUBS


def dot_nn(a, b):
    return lax.dot_general(a, b, (((1,), (0,)), ((), ())), preferred_element_type=F32)


def dot_nt(a, b):
    return lax.dot_general(a, b, (((1,), (1,)), ((), ())), preferred_element_type=F32)


def split3(x):
    hi = x.astype(BF16)
    rest = x - hi.astype(F32)
    mid = rest.astype(BF16)
    low = (rest - mid.astype(F32)).astype(BF16)
    return hi, mid, low


def iota(shape, dim):
    return lax.broadcasted_iota(jnp.int32, shape, dim)


def kernel(feats_h, w_one_h, w_two_h, idx_h, cnt_h, src_h, wt_h, lab_h, mask_h,
           outs, count_ref,
           idx_ref, cnt_ref, src_ref, wt_ref, lab_ref, mask_ref,
           feats_raw, feats_t, w_one_f, w_two_f, w_two_p, w_two_3, w_one_t, wts, row_ids, at_0, at_1, sel,
           z1_acc, z1_t, z2_acc, z2_s, h1_t, x1, halo1, x2, halo2, th, tret, cnt_src, cnt_in,
           grads, a_in, b_out, b_in,
           in_sem, s1, r1, sc, rc, s2, r2, s3, r3, sa, ra, sb, rb, so, ro, sd, rd):
    me = lax.axis_index("graph")
    core = me % 2
    chip = me // 2
    cx = chip % 2
    cy = chip // 2

    def flip_chip(f):
        fx, fy = f % 2, f // 2
        nx = 1 - cx if fx else cx
        ny = 1 - cy if fy else cy
        return ny * 2 + nx

    def flip_dev(f):
        nc = 1 - core if f % 2 else core
        return flip_chip(f // 2) * 2 + nc

    peers = [flip_dev(f) for f in SLOTS]

    barrier = pltpu.get_barrier_semaphore()
    for peer in peers:
        pl.semaphore_signal(barrier, inc=1, device_id=(peer,), device_id_type=MESH)

    pairs = [(idx_h, idx_ref), (cnt_h, cnt_ref), (feats_h, feats_raw), (src_h, src_ref), (wt_h, wt_ref),
             (mask_h, mask_ref), (lab_h, lab_ref), (w_one_h, w_one_f), (w_two_h, w_two_f)]
    loads = [pltpu.make_async_copy(a, b, in_sem.at[n]) for n, (a, b) in enumerate(pairs)]
    for load in loads:
        load.start()
    ats = [at_0, at_1]

    def number_rows(i, carry):
        start = pl.multiple_of(i * 32, 32)
        row_ids[pl.ds(start, 32), :] = iota((32, LANE), 0) + start
        return carry

    lax.fori_loop(0, ROWS // 32, number_rows, 0)
    for p, peer in enumerate(peers):
        def number_halo(i, carry, p=p, peer=peer):
            start = pl.multiple_of(i * 32, 32)
            row_ids[pl.ds(ROWS + p * HALO + start, 32), :] = iota((32, LANE), 0) + (ROWS + peer * HALO + start)
            return carry

        lax.fori_loop(0, HALO // 32, number_halo, 0)

    loads[0].wait()
    loads[1].wait()
    eye = iota((HALO, HALO), 0) == iota((HALO, HALO), 1)
    for p, peer in enumerate(peers):
        row = jnp.where(iota((1, HALO), 1) < cnt_ref[peer], idx_ref[pl.ds(peer, 1), :], -1).astype(F32)
        col = jnp.sum(jnp.where(eye, jnp.broadcast_to(row, (HALO, HALO)), 0.0), axis=1, keepdims=True)
        col = col.astype(jnp.int32)
        hot = iota((HALO, ROWS), 1) == jnp.broadcast_to(col, (HALO, ROWS))
        sel[pl.ds(p * HALO, HALO), :] = jnp.where(hot, 1.0, 0.0).astype(BF16)

    loads[5].wait()
    mask_f = mask_ref[...].astype(F32)
    own_count = jnp.sum(mask_f, axis=1, keepdims=True)
    cnt_src[...] = jnp.broadcast_to(own_count, (8, LANE))

    loads[3].wait()
    loads[4].wait()
    src = src_ref[...]
    wt = wt_ref[...]
    krow = iota((DEG, ROWS), 0)
    total = wt
    for d in range(1, DEG):
        same = (pltpu.roll(src, d, 0) == src) & (krow >= d)
        total = total + jnp.where(same, pltpu.roll(wt, d, 0), 0.0)
    wts[...] = total

    def build(t, lane, start, count, step=32):
        lanes = pl.ds(pl.multiple_of(t * TILE + lane * LANE, LANE), LANE)
        source = src_ref[:, lanes]
        weight = wts[:, lanes]
        sources = [jnp.broadcast_to(source[k:k + 1, :], (step, LANE)) for k in range(DEG)]
        weights = [jnp.broadcast_to(weight[k:k + 1, :], (step, LANE)) for k in range(DEG)]
        for piece in range(count // step):
            here = pl.ds(pl.multiple_of(start + piece * step, step), step)
            rows = row_ids[here, :]
            acc = jnp.zeros((step, LANE), F32)
            for k in range(DEG):
                acc = jnp.where(rows == sources[k], weights[k], acc)
            for n, term in enumerate(split3(acc)):
                ats[t][n, here, pl.ds(pl.multiple_of(lane * LANE, LANE), LANE)] = term

    def build_local(t, begin, end):
        def stage(i, carry):
            build(t, i // 2, pl.multiple_of((i % 2) * 512, 512), 512)
            return carry

        lax.fori_loop(begin, end, stage, 0)

    def build_halo(t):
        def stage(i, carry):
            build(t, i, ROWS, HALOS)
            return carry

        lax.fori_loop(0, 4, stage, 0)

    def aggregate(left, first, count, t):
        rows = pl.ds(first, count)
        return (dot_nn(left, ats[t][0, rows, :]) + dot_nn(left, ats[t][1, rows, :])
                + dot_nn(left, ats[t][2, rows, :]))

    def cols_of(t):
        return pl.ds(t * TILE, TILE)

    build_local(0, 0, AHEAD)

    loads[2].wait()
    feats_t[pl.ds(592, FEAT_L - 592), :] = jnp.zeros((FEAT_L - 592, ROWS), BF16)
    feats_t[pl.ds(0, FEAT), :] = feats_raw[...]

    def exchange(src, dst, send, recv):
        return [pltpu.make_async_remote_copy(
            src_ref=src.at[pl.ds(p * HALO, HALO), :], dst_ref=dst.at[pl.ds(p * HALO, HALO), :],
            send_sem=send.at[p], recv_sem=recv.at[p], device_id=(peer,), device_id_type=MESH)
            for p, peer in enumerate(peers)]

    early = pl.ds(0, EARLY * HALO)
    late = pl.ds(EARLY * HALO, HALOS - EARLY * HALO)
    ex1 = exchange(x1, halo1, s1, r1)
    x1[early, :] = dot_nt(sel[early, :], feats_t[...]).astype(BF16)
    pl.semaphore_wait(barrier, DEVS - 1)
    for p in range(EARLY):
        ex1[p].start()
    x1[late, :] = dot_nt(sel[late, :], feats_t[...]).astype(BF16)
    loads[7].wait()
    w_one_t[:, pl.ds(512, FEAT_P - 512)] = jnp.zeros((HID, FEAT_P - 512), BF16)
    w_one_t[:, pl.ds(0, FEAT)] = w_one_f[...].T.astype(BF16)
    for p in range(EARLY, DEVS - 1):
        ex1[p].start()
    counts = []
    for p, peer in enumerate(peers):
        counts.append(pltpu.make_async_remote_copy(
            src_ref=cnt_src, dst_ref=cnt_in.at[p], send_sem=sc.at[p], recv_sem=rc.at[p],
            device_id=(peer,), device_id_type=MESH))
        counts[-1].start()

    for t in range(TILES):
        build_local(t, 0 if t else AHEAD, 8)
        z1_acc[:, cols_of(t)] = aggregate(feats_t[pl.ds(0, FEAT_P), :], 0, ROWS, t)

    for t in range(TILES):
        build_halo(t)

    for p in range(EARLY):
        ex1[p].wait_recv()
    halo1_t = halo1[early, :].T[:FEAT_P, :]
    for t in range(TILES):
        z1_acc[:, cols_of(t)] = z1_acc[:, cols_of(t)] + aggregate(halo1_t, ROWS, EARLY * HALO, t)
    for p in range(EARLY, DEVS - 1):
        ex1[p].wait_recv()
    halo1_t = halo1[late, :].T[:FEAT_P, :]
    for t in range(TILES):
        z1_t[:, cols_of(t)] = (z1_acc[:, cols_of(t)] + aggregate(
            halo1_t, ROWS + EARLY * HALO, HALOS - EARLY * HALO, t)).astype(BF16)

    h1_t[...] = jnp.maximum(dot_nn(w_one_t[...], z1_t[...]), 0.0).astype(BF16)
    ex2 = exchange(x2, halo2, s2, r2)
    x2[early, :] = dot_nt(sel[early, :], h1_t[...]).astype(BF16)
    for copy in ex2[:EARLY]:
        copy.start()
    x2[late, :] = dot_nt(sel[late, :], h1_t[...]).astype(BF16)
    for copy in ex2[EARLY:]:
        copy.start()

    loads[6].wait()
    loads[8].wait()
    w_two_p[...] = jnp.zeros((CLS_P, HID), BF16)
    w_two_p[pl.ds(0, CLS), :] = w_two_f[...].astype(BF16)
    w_two_b = w_two_p[...]
    w_two_3[...] = jnp.concatenate([w_two_b.astype(F32)] * 3, axis=0).T.astype(BF16)
    for t in range(TILES):
        z2_acc[:, cols_of(t)] = aggregate(h1_t[...], 0, ROWS, t)
    for copy in ex2:
        copy.wait_recv()
    halo2_t = halo2[...].T
    for t in range(TILES):
        z2_s[:, cols_of(t)] = (z2_acc[:, cols_of(t)] + aggregate(halo2_t, ROWS, HALOS, t)).astype(BF16)
    z2_t = z2_s[...]

    count = cnt_src[...]
    for p in range(DEVS - 1):
        counts[p].wait_recv()
        count = count + cnt_in[p]
    count = count[0:1, 0:1]

    logits = dot_nn(w_two_b, z2_t)
    cls_row = iota((CLS_P, ROWS), 0)
    real = cls_row < CLS
    top = jnp.max(jnp.where(real, logits, -3.0e38), axis=0, keepdims=True)
    shifted = logits - top
    expo = jnp.where(real, jnp.exp(shifted), 0.0)
    log_prob = shifted - jnp.log(jnp.sum(expo, axis=0, keepdims=True))
    hit = cls_row == lab_ref[...]
    loss_row = jnp.sum(jnp.where(hit, log_prob, 0.0), axis=0, keepdims=True) * mask_f
    scale = mask_f / count
    d_log = (jnp.exp(log_prob) - jnp.where(hit, 1.0, 0.0)) * scale
    g2_t = jnp.where(real, d_log, 0.0).astype(BF16)

    def scatter(first, rows_n):
        rows = pl.ds(first, rows_n)
        out = jnp.zeros((CLS_P, rows_n), F32)
        for t in range(TILES):
            for n in range(3):
                out = out + dot_nt(g2_t[:, t * TILE:(t + 1) * TILE], ats[t][n, rows, :])
        return out

    th[:, pl.ds(0, HALOS)] = scatter(ROWS, HALOS)
    th[:, pl.ds(HALOS, HALO)] = jnp.zeros((CLS_P, HALO), F32)
    ex3 = [pltpu.make_async_remote_copy(
        src_ref=th.at[:, pl.ds(p // 2 * LANE, LANE)], dst_ref=tret.at[p],
        send_sem=s3.at[p], recv_sem=r3.at[p], device_id=(peer,), device_id_type=MESH)
        for p, peer in enumerate(peers)]
    for copy in ex3:
        copy.start()

    own_t = scatter(0, ROWS)
    grad_two = dot_nt(g2_t, z2_t)
    loss_sum = jnp.sum(loss_row, axis=1, keepdims=True)
    grad_two = jnp.where(iota((CLS_P, HID), 0) == CLS, jnp.broadcast_to(loss_sum, (CLS_P, HID)), grad_two)

    for copy in ex3:
        copy.wait_recv()
    first_half = iota((CLS_P, LANE), 1) < HALO
    blocks = [jnp.where(first_half, tret[2 * n], tret[2 * n + 1] if n < 3 else 0.0) for n in range(4)]
    back_t = jnp.concatenate(blocks, axis=1)[:, :HALOS]
    back = dot_nn(jnp.concatenate(split3(back_t), axis=0), sel[...])
    own_t = own_t + (back[0:CLS_P] + back[CLS_P:2 * CLS_P] + back[2 * CLS_P:3 * CLS_P])
    d_h1 = dot_nn(w_two_3[...], jnp.concatenate(split3(own_t), axis=0))
    g1_b = jnp.where(h1_t[...].astype(F32) > 0, d_h1, 0.0).astype(BF16)
    half_m = FEAT_P // 2
    grad_one = jnp.concatenate([dot_nt(z1_t[pl.ds(0, half_m), :], g1_b),
                                dot_nt(z1_t[pl.ds(half_m, half_m), :], g1_b)], axis=0)

    for h in range(2):
        lanes = slice(h * LANE, (h + 1) * LANE)
        for j in range(3):
            grads[h, j] = grad_one[j * OUT_SH:(j + 1) * OUT_SH, lanes]
        grads[h, 3, pl.ds(0, FEAT_P - 3 * OUT_SH), :] = grad_one[3 * OUT_SH:FEAT_P, lanes]
        grads[h, 3, pl.ds(FEAT_P - 3 * OUT_SH, CLS_P), :] = grad_two[:, lanes]
        grads[h, 3, pl.ds(FEAT_P - 3 * OUT_SH + CLS_P, 16), :] = jnp.zeros((16, LANE), F32)

    mate = flip_dev(1)
    flips = [3, 1, 2]

    def part(u):
        return pl.ds(u * SUB, SUB)

    copy_a, copy_b, copy_c, copy_d = {}, {}, {}, {}
    for u in range(SUBS):
        for o in flips + [0]:
            to_chip = flip_chip(o)
            copy_a[o, u] = pltpu.make_async_remote_copy(
                src_ref=grads.at[1 - core, to_chip, part(u), :], dst_ref=a_in.at[o, part(u), :],
                send_sem=sa.at[o, u], recv_sem=ra.at[o, u], device_id=(mate,), device_id_type=MESH)
            copy_a[o, u].start()
    for u in range(SUBS):
        for o in flips:
            to_chip = flip_chip(o)
            copy_a[o, u].wait_recv()
            b_out[o, part(u), :] = grads[core, to_chip, part(u), :] + a_in[o, part(u), :]
            copy_b[o, u] = pltpu.make_async_remote_copy(
                src_ref=b_out.at[o, part(u), :], dst_ref=b_in.at[o, part(u), :],
                send_sem=sb.at[o, u], recv_sem=rb.at[o, u],
                device_id=(to_chip * 2 + core,), device_id_type=MESH)
            copy_b[o, u].start()

    def to_mate(o, u):
        at_chip = flip_chip(o)
        copy_d[o, u] = pltpu.make_async_remote_copy(
            src_ref=outs.at[core, at_chip, part(u), :], dst_ref=outs.at[core, at_chip, part(u), :],
            send_sem=sd.at[o, u], recv_sem=rd.at[o, u], device_id=(mate,), device_id_type=MESH)
        copy_d[o, u].start()

    for u in range(SUBS):
        copy_a[0, u].wait_recv()
        mine = grads[core, chip, part(u), :] + a_in[0, part(u), :]
        for o in flips:
            copy_b[o, u].wait_recv()
        outs[core, chip, part(u), :] = mine + (
            (b_in[1, part(u), :] + b_in[2, part(u), :]) + b_in[3, part(u), :])
        for o in flips:
            copy_c[o, u] = pltpu.make_async_remote_copy(
                src_ref=outs.at[core, chip, part(u), :], dst_ref=outs.at[core, chip, part(u), :],
                send_sem=so.at[o, u], recv_sem=ro.at[o, u],
                device_id=(flip_chip(o) * 2 + core,), device_id_type=MESH)
            copy_c[o, u].start()
        to_mate(0, u)
    for u in range(SUBS):
        for o in [1, 2, 3]:
            copy_c[o, u].wait_recv()
            to_mate(o, u)
    for u in range(SUBS):
        for o in [0, 1, 2, 3]:
            copy_d[o, u].wait_recv()

    count_ref[...] = jnp.broadcast_to(count, (8, LANE))

    for copy in ex1 + ex2 + ex3 + counts:
        copy.wait_send()
    for group in (copy_a, copy_b, copy_c, copy_d):
        for copy in group.values():
            copy.wait_send()


def lay_out(outs, count_ref, loss_ref, g1_ref, g2_ref):
    for h in range(2):
        lanes = pl.ds(h * LANE, LANE)
        for j in range(3):
            g1_ref[pl.ds(j * OUT_SH, OUT_SH), lanes] = outs[h, j]
        g1_ref[pl.ds(3 * OUT_SH, FEAT - 3 * OUT_SH), lanes] = outs[h, 3, 0:FEAT - 3 * OUT_SH, :]
        g2_ref[:, lanes] = outs[h, 3, FEAT_P - 3 * OUT_SH:FEAT_P - 3 * OUT_SH + CLS, :]
    loss_at = FEAT_P - 3 * OUT_SH + CLS
    loss_ref[...] = -outs[0, 3, loss_at:loss_at + 1, 0:1] / count_ref[0:1, 0:1]


def solution(mesh):
    vmem = pl.BlockSpec(memory_space=pltpu.VMEM)
    hbm = pl.BlockSpec(memory_space=pl.ANY)
    dma8 = pltpu.SemaphoreType.DMA((8,))
    dma_sum = pltpu.SemaphoreType.DMA((4, SUBS))

    def device_step(feats, w_one, w_two, send_idx, send_count, edge_src, edge_wt, labels, label_mask):
        call = pl.pallas_call(
            kernel,
            out_shape=(pltpu.VMEM((2, 4, OUT_SH, LANE), F32), pltpu.VMEM((8, LANE), F32)),
            in_specs=[hbm] * 9,
            out_specs=(vmem, vmem),
            scratch_shapes=[
                pltpu.VMEM((DEVS, HALO), jnp.int32), pltpu.SMEM((DEVS,), jnp.int32),
                pltpu.VMEM((DEG, ROWS), jnp.int32), pltpu.VMEM((DEG, ROWS), F32),
                pltpu.VMEM((1, ROWS), jnp.int32), pltpu.VMEM((1, ROWS), jnp.int32),
                pltpu.VMEM((FEAT, ROWS), BF16), pltpu.VMEM((FEAT_L, ROWS), BF16), pltpu.VMEM((FEAT, HID), F32),
                pltpu.VMEM((CLS, HID), F32), pltpu.VMEM((CLS_P, HID), BF16), pltpu.VMEM((HID, 3 * CLS_P), BF16),
                pltpu.VMEM((HID, FEAT_P), BF16), pltpu.VMEM((DEG, ROWS), F32), pltpu.VMEM((EXT, LANE), jnp.int32),
                pltpu.VMEM((3, EXT, TILE), BF16), pltpu.VMEM((3, EXT, TILE), BF16),
                pltpu.VMEM((HALOS, ROWS), BF16),
                pltpu.VMEM((FEAT_P, ROWS), F32), pltpu.VMEM((FEAT_P, ROWS), BF16),
                pltpu.VMEM((HID, ROWS), F32), pltpu.VMEM((HID, ROWS), BF16),
                pltpu.VMEM((HID, ROWS), BF16),
                pltpu.VMEM((HALOS, FEAT_L), BF16), pltpu.VMEM((HALOS, FEAT_L), BF16),
                pltpu.VMEM((HALOS, HID), BF16), pltpu.VMEM((HALOS, HID), BF16),
                pltpu.VMEM((CLS_P, 512), F32), pltpu.VMEM((7, CLS_P, LANE), F32),
                pltpu.VMEM((8, LANE), F32), pltpu.VMEM((8, 8, LANE), F32),
                pltpu.VMEM((2, 4, OUT_SH, LANE), F32), pltpu.VMEM((4, OUT_SH, LANE), F32),
                pltpu.VMEM((4, OUT_SH, LANE), F32), pltpu.VMEM((4, OUT_SH, LANE), F32),
                pltpu.SemaphoreType.DMA((9,)), dma8, dma8, dma8, dma8, dma8, dma8, dma8, dma8,
                dma_sum, dma_sum, dma_sum, dma_sum, dma_sum, dma_sum, dma_sum, dma_sum,
            ],
            compiler_params=pltpu.CompilerParams(
                collective_id=0, has_side_effects=True, vmem_limit_bytes=56 * 1024 * 1024),
            name="gcn_step",
        )
        outs, count = call(
            feats.T, w_one, w_two.T, send_idx, send_count, edge_src.T, edge_wt.T,
            labels.reshape(1, ROWS), label_mask.reshape(1, ROWS))
        loss, grad_one, grad_two = pl.pallas_call(
            lay_out,
            out_shape=(jax.ShapeDtypeStruct((1, 1), F32), jax.ShapeDtypeStruct((FEAT, HID), F32),
                       jax.ShapeDtypeStruct((CLS, HID), F32)),
            in_specs=[vmem, vmem], out_specs=(vmem, vmem, vmem), name="gcn_results",
        )(*(pltpu.with_memory_space_constraint(x, pltpu.VMEM) for x in (outs, count)))
        return loss.reshape(()), grad_one, grad_two.T

    row_spec = P("graph", None)
    vec_spec = P("graph")
    return jax.shard_map(
        device_step, mesh=mesh,
        in_specs=(row_spec, P(), P(), row_spec, vec_spec, row_spec, row_spec, vec_spec, vec_spec),
        out_specs=(P(), P(), P()), check_vma=False)
```
